32 devices in a mesh: dp: 2 (over z, core), tp: 16 (over x, y).
Axes of the slice: x: 4, y: 4, z: 1, core: 2. Of those that a mesh axis runs over, the one named last changes fastest.
The devices are a block of a 4x4x8 slice.
Arguments:
- x: bfloat16 [4096, 4096], P('dp'), parts along dimension 0
- dy: bfloat16 [4096, 4096], P('dp'), parts along dimension 0
- gate: bfloat16 [4096, 16384], P('dp', 'tp'), parts along dimension 0
- up: bfloat16 [4096, 16384], P('dp', 'tp'), parts along dimension 0
- w_gate: bfloat16 [4096, 16384], P(None, 'tp')
- w_up: bfloat16 [4096, 16384], P(None, 'tp')
- w_down: bfloat16 [16384, 4096], P('tp')
Outputs:
- output 1: bfloat16 [4096, 4096], P('dp'), parts along dimension 0
- output 2: bfloat16 [8192, 16384], P('dp', 'tp'), parts along dimension 0
- output 3: bfloat16 [8192, 16384], P('dp', 'tp'), parts along dimension 0
- output 4: bfloat16 [32768, 4096], P(('dp', 'tp')), parts along dimension 0
There are 2 independent parts. The reference program is written for one: setup_inputs(seed, part) draws one part's arguments, and reference() takes and returns one part's arrays. A program takes and returns all parts, laid end to end along the dimension named above; an argument that names none is the same for every part.
All inputs are finite; a program needn't handle non-finite values.
Results may differ from the reference program's by a relative error of at most 0.012.
Values are sent between devices in bfloat16 or wider.
A program may use at most 768 MiB of HBM per device.

```python
import jax
import jax.numpy as jnp

ROWS = 2048
D = 4096
FF = 16384


def act(gate, up):
    return jax.nn.silu(gate) * up


def setup_inputs(seed: int = 0, part: int = 0) -> dict:
    kx, ky, ka, kb, kg, ku, kd = jax.random.split(jax.random.key(seed), 7)
    kx, ky, ka, kb = (jax.random.fold_in(k, part) for k in (kx, ky, ka, kb))
    drawn = {
        "x": jax.random.normal(kx, (ROWS, D), jnp.float32),
        "dy": jax.random.normal(ky, (ROWS, D), jnp.float32),
        "gate": jax.random.normal(ka, (ROWS, FF), jnp.float32),
        "up": jax.random.normal(kb, (ROWS, FF), jnp.float32),
        "w_gate": jax.random.normal(kg, (D, FF), jnp.float32) * D**-0.5,
        "w_up": jax.random.normal(ku, (D, FF), jnp.float32) * D**-0.5,
        "w_down": jax.random.normal(kd, (FF, D), jnp.float32) * FF**-0.5,
    }
    return {k: v.astype(jnp.bfloat16) for k, v in drawn.items()}


def reference(x, dy, gate, up, w_gate, w_up, w_down):
    hidden, back = jax.vjp(act, gate.astype(jnp.float32), up.astype(jnp.float32))
    d_hidden = jnp.dot(dy, w_down.T, preferred_element_type=jnp.float32)
    d_gate, d_up = (g.astype(jnp.bfloat16) for g in back(d_hidden))
    dx = jnp.dot(d_gate, w_gate.T, preferred_element_type=jnp.float32) + jnp.dot(d_up, w_up.T, preferred_element_type=jnp.float32)
    dw_gate = jnp.dot(x.T, d_gate, preferred_element_type=jnp.float32)
    dw_up = jnp.dot(x.T, d_up, preferred_element_type=jnp.float32)
    dw_down = jnp.dot(hidden.astype(jnp.bfloat16).T, dy, preferred_element_type=jnp.float32)
    return tuple(g.astype(jnp.bfloat16) for g in (dx, dw_gate, dw_up, dw_down))
```

```python
import functools
import math

import jax
import jax.numpy as jnp
from jax import lax
from jax.experimental import pallas as pl
from jax.experimental.pallas import tpu as pltpu
from jax.sharding import PartitionSpec as P

MESH = pl.DeviceIdType.MESH
BF, F32 = jnp.bfloat16, jnp.float32
NT = (((1,), (1,)), ((), ()))
VMEM_LIMIT = 63 * 1024 * 1024
WAVE = 256


def reduce_kernel(side, dy_h, gate_h, up_h, wg_h, wu_h, wd_h, hid_h, dgu_h, a0_h, a1_h, b0_h, b1_h,
                  wd, wgu, dy, gate, up, dgu, hid, s_h1, s_n, r_h1, r_n, total, s_g1, s_gn, r_g1, r_gn, xb,
                  w_sem, in_sem, o_sem, xo_sem, ss_h1, ss_n, ss_g1, ss_gn, ss_f, ss_w, rs_h1, rs_n, rs_g1, rs_gn, rs_f, rs_w):
    rows, depth = dy_h.shape
    ff = hid_h.shape[1]
    wave = dy.shape[1]
    half = wave // 2
    waves = rows // wave
    block = depth // (2 * side)
    sub = block // side
    me = lax.axis_index("tp")
    px, py = lax.div(me, side), lax.rem(me, side)
    first, second = (px, py), (py, px)

    def at(pos, d):
        return lax.rem(pos + d + side, side)

    def peer(axis, d):
        return {"tp": at(px, d) * side + py if axis == 0 else px * side + at(py, d)}

    barrier = pltpu.get_barrier_semaphore()
    for axis in (0, 1):
        for d in (1, -1):
            pl.semaphore_signal(barrier, inc=1, device_id=peer(axis, d), device_id_type=MESH)
    pl.semaphore_wait(barrier, 4)

    TOP, BOT = pl.ds(0, half), pl.ds(half, half)
    HALVES = (TOP, BOT)
    STEP = (1, -1)

    def remote(src, dst, ss, rs, axis, d):
        return pltpu.make_async_remote_copy(src_ref=src, dst_ref=dst, send_sem=ss, recv_sem=rs,
                                            device_id=peer(axis, STEP[d]), device_id_type=MESH)

    def c_h1(w, s, d):
        return remote(s_h1.at[w % 2, s, HALVES[d]], r_h1.at[w % 4, s, d], ss_h1.at[w % 2, s, d], rs_h1.at[w % 4, s, d], s, d)

    def c_n(w, s, d):
        return remote(s_n.at[w % 2, s, d], r_n.at[w % 4, s, d], ss_n.at[w % 2, s, d], rs_n.at[w % 4, s, d], s, d)

    def c_g1(w, s, d):
        return remote(s_g1.at[w % 2, s, HALVES[d]], r_g1.at[w % 4, s, d], ss_g1.at[w % 2, s, d], rs_g1.at[w % 4, s, d], 1 - s, d)

    def c_gn(w, s, d):
        return remote(s_gn.at[w % 2, s, d], r_gn.at[w % 4, s, d], ss_gn.at[w % 2, s, d], rs_gn.at[w % 4, s, d], 1 - s, d)

    def cols(s, d):
        return pl.ds(pl.multiple_of(at(second[s], d) * sub, sub), sub)

    def c_f(w, s, d):
        own = xb.at[w % 4, s, :, cols(s, 0)]
        return remote(own, own, ss_f.at[w % 4, s, d], rs_f.at[w % 4, s, d], 1 - s, d)

    def c_w(w, s, d):
        got = xb.at[w % 4, s, HALVES[d], cols(s, -STEP[d])]
        return remote(got, got, ss_w.at[w % 4, s, d], rs_w.at[w % 4, s, d], 1 - s, d)

    def ins(w):
        r = pl.ds(pl.multiple_of(w * wave, wave), wave)
        k = w % 2
        return (pltpu.make_async_copy(dy_h.at[r], dy.at[k], in_sem.at[k, 0]),
                pltpu.make_async_copy(gate_h.at[r], gate.at[k], in_sem.at[k, 1]),
                pltpu.make_async_copy(up_h.at[r], up.at[k], in_sem.at[k, 2]))

    def outs(w):
        r = pl.ds(pl.multiple_of(w * wave, wave), wave)
        return (pltpu.make_async_copy(hid.at[w % 2], hid_h.at[r], o_sem.at[w % 2, 0]),
                pltpu.make_async_copy(dgu.at[w % 4], dgu_h.at[r], o_sem.at[w % 2, 1]))

    def xb_outs(w, refs):
        r = pl.ds(pl.multiple_of((w % (waves // 2)) * wave, wave), wave)
        return [pltpu.make_async_copy(xb.at[w % 4, s], refs[s].at[r], xo_sem.at[w % 4, s]) for s in (0, 1)]

    def weights(s, d):
        r = pl.ds(pl.multiple_of(s * side * block + at(first[s], d) * block, block), block)
        k = (d + side) % side
        return (pltpu.make_async_copy(wg_h.at[r], wgu.at[r, pl.ds(0, ff)], w_sem.at[s, k, 0]),
                pltpu.make_async_copy(wu_h.at[r], wgu.at[r, pl.ds(ff, ff)], w_sem.at[s, k, 1]))

    down = pltpu.make_async_copy(wd_h, wd, w_sem.at[2, 0, 0])
    for c in ins(0):
        c.start()
    down.start()

    def dot_block(w, s, d):
        r = pl.ds(pl.multiple_of(s * side * block + at(first[s], d) * block, block), block)
        return lax.dot_general(dgu[w % 4], wgu[r, :], NT, preferred_element_type=F32)

    def wait_weights(t, when, d):
        @pl.when(t == when)
        def _():
            for s in (0, 1):
                for c in weights(s, d):
                    c.wait()

    def stage(t, lag):
        w = t - lag
        return w, pl.when(jnp.logical_and(w >= 0, w < waves))

    def body(t, _):
        w7, active = stage(t, 7)

        @active
        def _():
            for c in xb_outs(w7, (a0_h, b0_h)):
                c.wait()

        w0, active = stage(t, 0)

        @active
        def _():
            @pl.when(w0 + 1 < waves)
            def _():
                for c in ins(w0 + 1):
                    c.start()
            for c in ins(w0):
                c.wait()

            @pl.when(w0 == 0)
            def _():
                down.wait()
                for d in (2, 1, -1, 0):
                    for s in (0, 1):
                        for c in weights(s, d):
                            c.start()

            @pl.when(w0 >= 2)
            def _():
                for c in outs(w0 - 2):
                    c.wait()
            k = w0 % 2
            dh = lax.dot_general(dy[k], wd[...], NT, preferred_element_type=F32)
            g, u = gate[k].astype(F32), up[k].astype(F32)
            sg = jax.nn.sigmoid(g)
            si = g * sg
            dgu[w0 % 4, :, 0:ff] = (dh * u * (sg * (1.0 + g * (1.0 - sg)))).astype(BF)
            dgu[w0 % 4, :, ff:2 * ff] = (dh * si).astype(BF)
            hid[k] = (si * u).astype(BF)
            for c in outs(w0):
                c.start()

        w1, active = stage(t, 1)

        @active
        def _():
            wait_weights(t, 1, 1)
            wait_weights(t, 1, -1)
            for d in (0, 1):
                for s in (0, 1):
                    @pl.when(w1 >= 2)
                    def _():
                        c_n(w1 - 2, s, d).wait_send()
                    term = dot_block(w1, s, STEP[d])
                    c_h1(w1, s, d).wait_recv()
                    got, other = HALVES[d], HALVES[1 - d]
                    s_n[w1 % 2, s, d, got] = (term[d * half:(d + 1) * half] + r_h1[w1 % 4, s, d].astype(F32)).astype(BF)
                    s_n[w1 % 2, s, d, other] = term[(1 - d) * half:(2 - d) * half].astype(BF)
                    c_n(w1, s, d).start()

        w2, active = stage(t, 2)

        @active
        def _():
            wait_weights(t, 2, 0)
            for s in (0, 1):
                @pl.when(w2 >= 2)
                def _():
                    for d in (0, 1):
                        c_g1(w2 - 2, s, d).wait_send()
                term = dot_block(w2, s, 0)
                for d in (0, 1):
                    c_n(w2, s, d).wait_recv()
                total[w2 % 4, s] = term + (r_n[w2 % 4, s, 0].astype(F32) + r_n[w2 % 4, s, 1].astype(F32))
                s_g1[w2 % 2, s] = total[w2 % 4, s, :, cols(s, 2)].astype(BF)
                for d in (0, 1):
                    c_g1(w2, s, d).start()

        @stage(t, 0)[1]
        def _():
            wait_weights(t, 0, 2)
            for s in (0, 1):
                @pl.when(w0 >= 2)
                def _():
                    for d in (0, 1):
                        c_h1(w0 - 2, s, d).wait_send()
                s_h1[w0 % 2, s] = dot_block(w0, s, 2).astype(BF)
                for d in (0, 1):
                    c_h1(w0, s, d).start()

        w3, active = stage(t, 3)

        @active
        def _():
            for s in (0, 1):
                for d in (0, 1):
                    @pl.when(w3 >= 2)
                    def _():
                        c_gn(w3 - 2, s, d).wait_send()
                    c_g1(w3, s, d).wait_recv()
                    got, other = HALVES[d], HALVES[1 - d]
                    where = cols(s, STEP[d])
                    s_gn[w3 % 2, s, d, got] = (total[w3 % 4, s, got, where] + r_g1[w3 % 4, s, d].astype(F32)).astype(BF)
                    s_gn[w3 % 2, s, d, other] = total[w3 % 4, s, other, where].astype(BF)
                    c_gn(w3, s, d).start()

        w4, active = stage(t, 4)

        @active
        def _():
            for s in (0, 1):
                for d in (0, 1):
                    c_gn(w4, s, d).wait_recv()
                xb[w4 % 4, s, :, cols(s, 0)] = (
                    total[w4 % 4, s, :, cols(s, 0)] + (r_gn[w4 % 4, s, 0].astype(F32) + r_gn[w4 % 4, s, 1].astype(F32))).astype(BF)
                for d in (0, 1):
                    c_f(w4, s, d).start()

        w5, active = stage(t, 5)

        @active
        def _():
            for s in (0, 1):
                for d in (0, 1):
                    c_f(w5, s, d).wait_recv()
                for d in (0, 1):
                    c_w(w5, s, d).start()

        w6, active = stage(t, 6)

        @active
        def _():
            for s in (0, 1):
                for d in (0, 1):
                    c_w(w6, s, d).wait_recv()
                    c_w(w6, s, d).wait_send()
                    c_f(w6, s, d).wait_send()

            @pl.when(w6 < waves // 2)
            def _():
                for c in xb_outs(w6, (a0_h, b0_h)):
                    c.start()

            @pl.when(w6 >= waves // 2)
            def _():
                for c in xb_outs(w6, (a1_h, b1_h)):
                    c.start()
        return 0

    lax.fori_loop(0, waves + 7, body, 0)
    for w in (waves - 2, waves - 1):
        for c in outs(w):
            c.wait()
        for s in (0, 1):
            for d in (0, 1):
                c_h1(w, s, d).wait_send()
                c_n(w, s, d).wait_send()
                c_g1(w, s, d).wait_send()
                c_gn(w, s, d).wait_send()


def reduce_terms(side, dy, gate, up, w_gate, w_up, w_down):
    rows, depth = dy.shape
    ff = gate.shape[1]
    wave, half = WAVE, WAVE // 2
    block = depth // (2 * side)
    sub = block // side
    any_ = pl.BlockSpec(memory_space=pl.ANY)
    piece = jax.ShapeDtypeStruct((rows // 2, block), BF)
    V, DMA = pltpu.VMEM, pltpu.SemaphoreType.DMA
    return pl.pallas_call(
        functools.partial(reduce_kernel, side),
        out_shape=[jax.ShapeDtypeStruct((rows, ff), BF), jax.ShapeDtypeStruct((rows, 2 * ff), BF), piece, piece, piece, piece],
        in_specs=[any_] * 6,
        out_specs=[any_] * 6,
        scratch_shapes=[
            V((ff, depth), BF), V((depth, 2 * ff), BF), V((2, wave, depth), BF), V((2, wave, ff), BF), V((2, wave, ff), BF),
            V((4, wave, 2 * ff), BF), V((2, wave, ff), BF),
            V((2, 2, wave, block), BF), V((2, 2, 2, wave, block), BF), V((4, 2, 2, half, block), BF), V((4, 2, 2, wave, block), BF),
            V((4, 2, wave, block), F32),
            V((2, 2, wave, sub), BF), V((2, 2, 2, wave, sub), BF), V((4, 2, 2, half, sub), BF), V((4, 2, 2, wave, sub), BF),
            V((4, 2, wave, block), BF),
            DMA((3, side, 2)), DMA((2, 3)), DMA((2, 2)), DMA((4, 2)),
            DMA((2, 2, 2)), DMA((2, 2, 2)), DMA((2, 2, 2)), DMA((2, 2, 2)), DMA((4, 2, 2)), DMA((4, 2, 2)),
            DMA((4, 2, 2)), DMA((4, 2, 2)), DMA((4, 2, 2)), DMA((4, 2, 2)), DMA((4, 2, 2)), DMA((4, 2, 2)),
        ],
        compiler_params=pltpu.CompilerParams(collective_id=0, has_side_effects=True, vmem_limit_bytes=VMEM_LIMIT),
        cost_estimate=pl.CostEstimate(flops=6 * rows * depth * ff, bytes_accessed=2 * (rows * depth + 7 * rows * ff + 3 * ff * depth), transcendentals=0),
        name="reduce_terms",
    )(dy, gate, up, w_gate, w_up, w_down)


def gate_up_kernel(x, dgu, og, ou):
    ff = og.shape[1]
    xt = x[...].T
    og[...] = jnp.dot(xt, dgu[:, 0:ff], preferred_element_type=F32).astype(BF)
    ou[...] = jnp.dot(xt, dgu[:, ff:2 * ff], preferred_element_type=F32).astype(BF)


def grad_gate_up(x, dgu, tile=512):
    rows, depth = x.shape
    ff = dgu.shape[1] // 2
    return pl.pallas_call(
        gate_up_kernel,
        grid=(depth // tile,),
        in_specs=[pl.BlockSpec((rows, tile), lambda i: (0, i)), pl.BlockSpec((rows, 2 * ff), lambda i: (0, 0))],
        out_specs=[pl.BlockSpec((tile, ff), lambda i: (i, 0))] * 2,
        out_shape=[jax.ShapeDtypeStruct((depth, ff), BF)] * 2,
        cost_estimate=pl.CostEstimate(flops=4 * rows * depth * ff, bytes_accessed=2 * (rows * depth + 2 * rows * ff + 2 * depth * ff), transcendentals=0),
        compiler_params=pltpu.CompilerParams(vmem_limit_bytes=VMEM_LIMIT),
        name="grad_gate_up",
    )(x, dgu)


def placed(side, dx, where, block):
    me = lax.axis_index("tp")
    pos = (lax.div(me, side), lax.rem(me, side))
    h = dx.shape[0] // 2
    res = []
    for s, part, d in where:
        col = (s * side + lax.rem(pos[s] + d + side, side)) * block
        res.append(dx.at[pl.ds(part * h, h), pl.ds(pl.multiple_of(col, block), block)])
    return res


def down_kernel(side, where, hid, dy, *refs):
    n = len(where)
    src, (out, dx, buf, sem) = refs[:n], refs[n:]
    i = pl.program_id(0)
    got = [pltpu.make_async_copy(src[k], buf.at[k], sem.at[0, k]) for k in range(n)]
    put = [pltpu.make_async_copy(buf.at[k], r, sem.at[1, k]) for k, r in enumerate(placed(side, dx, where, buf.shape[2]))]

    @pl.when(i == 0)
    def _():
        for c in got:
            c.start()

    @pl.when(i == 2)
    def _():
        for c, p in zip(got, put):
            c.wait()
            p.start()
    out[...] = lax.dot_general(hid[...], dy[...], (((0,), (0,)), ((), ())), preferred_element_type=F32).astype(BF)

    @pl.when(i == pl.num_programs(0) - 1)
    def _():
        for p in put:
            p.wait()


def grad_down(side, hid, dy, pieces, where, tile=512):
    rows, depth = dy.shape
    ff = hid.shape[1]
    any_ = pl.BlockSpec(memory_space=pl.ANY)
    n = len(pieces)
    return pl.pallas_call(
        functools.partial(down_kernel, side, where),
        grid=(depth // tile,),
        in_specs=[pl.BlockSpec((rows, ff), lambda i: (0, 0)), pl.BlockSpec((rows, tile), lambda i: (0, i))] + [any_] * n,
        out_specs=[pl.BlockSpec((ff, tile), lambda i: (0, i)), any_],
        out_shape=[jax.ShapeDtypeStruct((ff, depth), BF), jax.ShapeDtypeStruct((rows, depth), BF)],
        scratch_shapes=[pltpu.VMEM((n, *pieces[0].shape), BF), pltpu.SemaphoreType.DMA((2, n))],
        cost_estimate=pl.CostEstimate(flops=2 * rows * depth * ff, bytes_accessed=2 * (2 * rows * depth + rows * ff + depth * ff), transcendentals=0),
        compiler_params=pltpu.CompilerParams(vmem_limit_bytes=VMEM_LIMIT),
        name="grad_down",
    )(hid, dy, *pieces)


def finish_kernel(side, where, *refs):
    n = len(where)
    src, (_, dx, buf, sem) = refs[:n], refs[n:]
    got = [pltpu.make_async_copy(src[k], buf.at[k], sem.at[0, k]) for k in range(n)]
    put = [pltpu.make_async_copy(buf.at[k], r, sem.at[1, k]) for k, r in enumerate(placed(side, dx, where, buf.shape[2]))]
    for c in got:
        c.start()
    for c, p in zip(got, put):
        c.wait()
        p.start()
    for p in put:
        p.wait()


def finish(side, dx, pieces, where):
    any_ = pl.BlockSpec(memory_space=pl.ANY)
    n = len(pieces)
    return pl.pallas_call(
        functools.partial(finish_kernel, side, where),
        in_specs=[any_] * (n + 1),
        out_specs=any_,
        out_shape=jax.ShapeDtypeStruct(dx.shape, BF),
        input_output_aliases={n: 0},
        scratch_shapes=[pltpu.VMEM((n, *pieces[0].shape), BF), pltpu.SemaphoreType.DMA((2, n))],
        cost_estimate=pl.CostEstimate(flops=1000000, bytes_accessed=2 * 2 * n * pieces[0].size, transcendentals=0),
        compiler_params=pltpu.CompilerParams(vmem_limit_bytes=VMEM_LIMIT),
        name="finish",
    )(*pieces, dx)


def solution(mesh):
    size = mesh.shape["tp"]
    side = math.isqrt(size)

    def ring(axis, d):
        def to(i):
            x, y = divmod(i, side)
            return ((x + d) % side) * side + y if axis == 0 else x * side + (y + d) % side
        return [(i, to(i)) for i in range(size)]

    def step(x, dy, gate, up, w_gate, w_up, w_down):
        hid, dgu, *own = reduce_terms(side, dy, gate, up, w_gate, w_up, w_down)
        own = ((own[0], own[1]), (own[2], own[3]))

        def send(v, s, d):
            return lax.ppermute(v, "tp", perm=ring(s, d))
        early = [(send(own[0][0], 0, 1), (0, 0, -1)), (send(own[1][0], 1, 1), (1, 0, -1)),
                 (send(own[0][1], 0, -1), (0, 1, 1)), (send(own[1][1], 1, -1), (1, 1, 1))]
        late = [(send(own[0][1], 0, 1), (0, 1, -1)), (send(own[1][1], 1, 1), (1, 1, -1)),
                (send(own[0][0], 0, -1), (0, 0, 1)), (send(own[1][0], 1, -1), (1, 0, 1))]
        dw_gate, dw_up = grad_gate_up(x, dgu)
        arrived, dw_gate, dw_up, hid = lax.optimization_barrier(([v for v, _ in early], dw_gate, dw_up, hid))
        early = [(v, k) for v, (_, k) in zip(arrived, early)]
        far = [(send(early[0][0], 0, 1), (0, 0, 2)), (send(early[1][0], 1, 1), (1, 0, 2)),
               (send(early[2][0], 0, -1), (0, 1, 2)), (send(early[3][0], 1, -1), (1, 1, 2))]
        mine = [(own[0][0], (0, 0, 0)), (own[0][1], (0, 1, 0)), (own[1][0], (1, 0, 0)), (own[1][1], (1, 1, 0))]
        dw_down, dx = grad_down(side, hid, dy, [v for v, _ in mine + early], [k for _, k in mine + early])
        dx = finish(side, dx, [v for v, _ in late + far], [k for _, k in late + far])
        return dx, dw_gate, dw_up, dw_down

    tokens, columns, rows = P("dp", None), P(None, "tp"), P("tp", None)
    return jax.shard_map(
        step,
        mesh=mesh,
        in_specs=(tokens, tokens, P("dp", "tp"), P("dp", "tp"), columns, columns, rows),
        out_specs=(tokens, P("dp", "tp"), P("dp", "tp"), P(("dp", "tp"), None)),
        check_vma=False,
    )
```

```python
import functools
import math

import jax
import jax.numpy as jnp
from jax import lax
from jax.experimental import pallas as pl
from jax.experimental.pallas import tpu as pltpu
from jax.sharding import PartitionSpec as P

MESH = pl.DeviceIdType.MESH
BF, F32 = jnp.bfloat16, jnp.float32
NT = (((1,), (1,)), ((), ()))
VMEM_LIMIT = 63 * 1024 * 1024
WAVE = 256
AHEAD = 1
TILE = 512


def reduce_kernel(side, dy_h, gate_h, up_h, wg_h, wu_h, wd_h, dgu_h, dwd_h, dx_h, a0_h, a1_h, b0_h, b1_h,
                  wd, wgu, dy, gate, up, dgu, hid, s_h1, s_n, r_h1, r_n, total, s_g1, s_gn, r_g1, r_gn, xb, whole,
                  w_sem, in_sem, o_sem, xo_sem, ss_h1, ss_n, ss_g1, ss_gn, ss_f, ss_w, rs_h1, rs_n, rs_g1, rs_gn, rs_f, rs_w,
                  ss_a, rs_a, ss_e, rs_e, t_sem, u_sem):
    rows, depth = dy_h.shape
    ff = gate_h.shape[1]
    wave = dy.shape[1]
    half = wave // 2
    waves = rows // wave
    pass_on = ((a0_h, a1_h), (b0_h, b1_h))
    block = depth // (2 * side)
    sub = block // side
    me = lax.axis_index("tp")
    px, py = lax.div(me, side), lax.rem(me, side)
    first, second = (px, py), (py, px)

    def at(pos, d):
        return lax.rem(pos + d + side, side)

    def peer(axis, d):
        return {"tp": at(px, d) * side + py if axis == 0 else px * side + at(py, d)}

    TOP, BOT = pl.ds(0, half), pl.ds(half, half)
    HALVES = (TOP, BOT)
    STEP = (1, -1)

    def remote(src, dst, ss, rs, axis, d):
        return pltpu.make_async_remote_copy(src_ref=src, dst_ref=dst, send_sem=ss, recv_sem=rs,
                                            device_id=peer(axis, STEP[d]), device_id_type=MESH)

    def c_h1(w, s, d):
        return remote(s_h1.at[w % 2, s, HALVES[d]], r_h1.at[w % 4, s, d], ss_h1.at[w % 2, s, d], rs_h1.at[w % 4, s, d], s, d)

    def c_n(w, s, d):
        return remote(s_n.at[w % 2, s, d], r_n.at[w % 4, s, d], ss_n.at[w % 2, s, d], rs_n.at[w % 4, s, d], s, d)

    def c_g1(w, s, d):
        return remote(s_g1.at[w % 2, s, HALVES[d]], r_g1.at[w % 4, s, d], ss_g1.at[w % 2, s, d], rs_g1.at[w % 4, s, d], 1 - s, d)

    def c_gn(w, s, d):
        return remote(s_gn.at[w % 2, s, d], r_gn.at[w % 4, s, d], ss_gn.at[w % 2, s, d], rs_gn.at[w % 4, s, d], 1 - s, d)

    def cols(s, d):
        return pl.ds(pl.multiple_of(at(second[s], d) * sub, sub), sub)

    def c_f(w, s, d):
        own = xb.at[w, s, :, cols(s, 0)]
        return remote(own, own, ss_f.at[w, s, d], rs_f.at[w, s, d], 1 - s, d)

    def c_w(w, s, d):
        got = xb.at[w, s, HALVES[d], cols(s, -STEP[d])]
        return remote(got, got, ss_w.at[w, s, d], rs_w.at[w, s, d], 1 - s, d)

    def ins(w):
        r = pl.ds(pl.multiple_of(w * wave, wave), wave)
        k = w % 2
        return (pltpu.make_async_copy(dy_h.at[r], dy.at[k], in_sem.at[k, 0]),
                pltpu.make_async_copy(gate_h.at[r], gate.at[k], in_sem.at[k, 1]),
                pltpu.make_async_copy(up_h.at[r], up.at[k], in_sem.at[k, 2]))

    def outs(w):
        r = pl.ds(pl.multiple_of(w * wave, wave), wave)
        return (pltpu.make_async_copy(dgu.at[w % 4], dgu_h.at[r], o_sem.at[w % 2]),)

    def xb_outs(w):
        return [pltpu.make_async_copy(xb.at[w, s, HALVES[1 - d]], pass_on[s][d].at[0, w - AHEAD], xo_sem.at[w, s, d])
                for s in (0, 1) for d in (0, 1)]

    def c_e(w, s, d):
        return remote(xb.at[w, s, HALVES[d]], pass_on[s][d].at[1, w - AHEAD], ss_e.at[w, s, d], rs_e.at[w, s, d], s, d)

    def weights(s, d):
        r = pl.ds(pl.multiple_of(s * side * block + at(first[s], d) * block, block), block)
        k = (d + side) % side
        return (pltpu.make_async_copy(wg_h.at[r], wgu.at[r, pl.ds(0, ff)], w_sem.at[s, k, 0]),
                pltpu.make_async_copy(wu_h.at[r], wgu.at[r, pl.ds(ff, ff)], w_sem.at[s, k, 1]))

    part = ff // 2

    def down(c):
        r = pl.ds(c * part, part)
        return pltpu.make_async_copy(wd_h.at[r], wd.at[r], w_sem.at[2, 0, c])

    for c in ins(0):
        c.start()
    for c in (0, 1):
        down(c).start()
    for s in (0, 1):
        for c in weights(s, 2):
            c.start()

    barrier = pltpu.get_barrier_semaphore()
    for axis in (0, 1):
        for d in (1, -1):
            pl.semaphore_signal(barrier, inc=1, device_id=peer(axis, d), device_id_type=MESH)
    pl.semaphore_wait(barrier, 4)

    tiles = depth // TILE

    def tile_in(j):
        c = pl.ds(pl.multiple_of(j * TILE, TILE), TILE)
        return [pltpu.make_async_copy(dy_h.at[pl.ds(i * ff, ff), c], wd.at[:, tile_at(j, i)], t_sem.at[j % 2, i]) for i in range(rows // ff)]

    def tile_at(j, i):
        return pl.ds(pl.multiple_of(((j % 2) * (rows // ff) + i) * TILE, TILE), TILE)

    def tile_out(j):
        c = pl.ds(pl.multiple_of(j * TILE, TILE), TILE)
        return pltpu.make_async_copy(wd.at[:, out_at(j)], dwd_h.at[:, c], u_sem.at[j % 2])

    def out_at(j):
        return pl.ds(pl.multiple_of((2 * (rows // ff) + j % 2) * TILE, TILE), TILE)

    def where_x(s, d):
        return pl.ds(pl.multiple_of((s * side + at(first[s], d)) * block, block), block)

    def c_a(w, s, d, kind):
        ref = whole.at[w, HALVES[1 - d if kind == 1 else d], where_x(s, -STEP[d] if kind == 2 else 0)]
        return remote(ref, ref, ss_a.at[w, s, d, kind], rs_a.at[w, s, d, kind], s, d)

    def dot_block(w, s, d):
        r = pl.ds(pl.multiple_of(s * side * block + at(first[s], d) * block, block), block)
        return lax.dot_general(dgu[w % 4], wgu[r, :], NT, preferred_element_type=F32)

    def wait_weights(t, when, d):
        @pl.when(t == when)
        def _():
            for s in (0, 1):
                for c in weights(s, d):
                    c.wait()

    def stage(t, lag):
        w = t - lag
        return w, pl.when(jnp.logical_and(w >= 0, w < waves))

    def body(t, _):
        w0, active = stage(t, 0)

        @active
        def _():
            @pl.when(w0 + 1 < waves)
            def _():
                for c in ins(w0 + 1):
                    c.start()
            for c in ins(w0):
                c.wait()

            @pl.when(w0 >= 2)
            def _():
                for c in outs(w0 - 2):
                    c.wait()
            k = w0 % 2
            for p in (0, 1):
                @pl.when(w0 == 0)
                def _():
                    down(p).wait()
                    if p == 0:
                        for d in (1, -1, 0):
                            for s in (0, 1):
                                for c in weights(s, d):
                                    c.start()
                f = pl.ds(p * part, part)
                dh = lax.dot_general(dy[k], wd[f, :], NT, preferred_element_type=F32)
                g, u = gate[k, :, f].astype(F32), up[k, :, f].astype(F32)
                sg = jax.nn.sigmoid(g)
                si = g * sg
                dgu[w0 % 4, :, f] = (dh * u * (sg * (1.0 + g * (1.0 - sg)))).astype(BF)
                dgu[w0 % 4, :, pl.ds(ff + p * part, part)] = (dh * si).astype(BF)
                hid[pl.ds(pl.multiple_of(w0 * wave, wave), wave), f] = (si * u).astype(BF)
            for c in outs(w0):
                c.start()

            @pl.when(w0 == waves - 1)
            def _():
                for c in tile_in(0):
                    c.start()

        @stage(t, 0)[1]
        def _():
            wait_weights(t, 0, 2)
            for s in (0, 1):
                @pl.when(w0 >= 2)
                def _():
                    for d in (0, 1):
                        c_h1(w0 - 2, s, d).wait_send()
                s_h1[w0 % 2, s] = dot_block(w0, s, 2).astype(BF)
                for d in (0, 1):
                    c_h1(w0, s, d).start()

        w1, active = stage(t, 1)

        @active
        def _():
            wait_weights(t, 1, 1)
            wait_weights(t, 1, -1)
            for d in (0, 1):
                for s in (0, 1):
                    @pl.when(w1 >= 2)
                    def _():
                        c_n(w1 - 2, s, d).wait_send()
                    term = dot_block(w1, s, STEP[d])
                    c_h1(w1, s, d).wait_recv()
                    got, other = HALVES[d], HALVES[1 - d]
                    s_n[w1 % 2, s, d, got] = (term[d * half:(d + 1) * half] + r_h1[w1 % 4, s, d].astype(F32)).astype(BF)
                    s_n[w1 % 2, s, d, other] = term[(1 - d) * half:(2 - d) * half].astype(BF)
                    c_n(w1, s, d).start()

        w2, active = stage(t, 2)

        @active
        def _():
            wait_weights(t, 2, 0)
            for s in (0, 1):
                @pl.when(w2 >= 2)
                def _():
                    for d in (0, 1):
                        c_g1(w2 - 2, s, d).wait_send()
                term = dot_block(w2, s, 0)
                for d in (0, 1):
                    c_n(w2, s, d).wait_recv()
                total[w2 % 4, s] = term + (r_n[w2 % 4, s, 0].astype(F32) + r_n[w2 % 4, s, 1].astype(F32))
                s_g1[w2 % 2, s] = total[w2 % 4, s, :, cols(s, 2)].astype(BF)
                for d in (0, 1):
                    c_g1(w2, s, d).start()

        w3, active = stage(t, 3)

        @active
        def _():
            for s in (0, 1):
                for d in (0, 1):
                    @pl.when(w3 >= 2)
                    def _():
                        c_gn(w3 - 2, s, d).wait_send()
                    c_g1(w3, s, d).wait_recv()
                    got, other = HALVES[d], HALVES[1 - d]
                    where = cols(s, STEP[d])
                    s_gn[w3 % 2, s, d, got] = (total[w3 % 4, s, got, where] + r_g1[w3 % 4, s, d].astype(F32)).astype(BF)
                    s_gn[w3 % 2, s, d, other] = total[w3 % 4, s, other, where].astype(BF)
                    c_gn(w3, s, d).start()

        w4, active = stage(t, 4)

        @active
        def _():
            for s in (0, 1):
                for d in (0, 1):
                    c_gn(w4, s, d).wait_recv()
                xb[w4, s, :, cols(s, 0)] = (
                    total[w4 % 4, s, :, cols(s, 0)] + (r_gn[w4 % 4, s, 0].astype(F32) + r_gn[w4 % 4, s, 1].astype(F32))).astype(BF)
                for d in (0, 1):
                    c_f(w4, s, d).start()

        w5, active = stage(t, 5)

        @active
        def _():
            for s in (0, 1):
                for d in (0, 1):
                    c_f(w5, s, d).wait_recv()
                for d in (0, 1):
                    c_w(w5, s, d).start()

        w6, active = stage(t, 6)

        @active
        def _():
            for s in (0, 1):
                for d in (0, 1):
                    c_w(w6, s, d).wait_recv()
                    c_w(w6, s, d).wait_send()
                    c_f(w6, s, d).wait_send()

            @pl.when(w6 < AHEAD)
            def _():
                for s in (0, 1):
                    whole[w6, :, where_x(s, 0)] = xb[w6, s]

            @pl.when(w6 >= AHEAD)
            def _():
                for c in xb_outs(w6):
                    c.start()

        w7 = t - 7

        @pl.when(jnp.logical_and(w7 >= AHEAD, w7 < waves))
        def _():
            for s in (0, 1):
                for d in (0, 1):
                    c_e(w7, s, d).start()

        for w in range(AHEAD):
            @pl.when(t == waves + 1 + w)
            def _():
                for s in (0, 1):
                    for d in (0, 1):
                        c_a(w, s, d, 0).start()

            @pl.when(t == waves + 1 + AHEAD + w)
            def _():
                for s in (0, 1):
                    for d in (0, 1):
                        c_a(w, s, d, 1).start()
                for s in (0, 1):
                    for d in (0, 1):
                        c_a(w, s, d, 0).wait_recv()
                        c_a(w, s, d, 2).start()

        j = t - waves

        @pl.when(jnp.logical_and(j >= 0, j < tiles))
        def _():
            for c in tile_in(j):
                c.wait()

            @pl.when(j + 1 < tiles)
            def _():
                for c in tile_in(j + 1):
                    c.start()

            @pl.when(j >= 2)
            def _():
                tile_out(j - 2).wait()
            acc = 0
            for i in range(rows // ff):
                acc += lax.dot_general(hid[pl.ds(i * ff, ff), :], wd[:, tile_at(j, i)], (((0,), (0,)), ((), ())), preferred_element_type=F32)
            wd[:, out_at(j)] = acc.astype(BF)
            tile_out(j).start()
        return 0

    lax.fori_loop(0, waves + max(8, tiles), body, 0)
    for w in range(AHEAD):
        for s in (0, 1):
            for d in (0, 1):
                c_a(w, s, d, 1).wait_recv()
                c_a(w, s, d, 2).wait_recv()
                for kind in (0, 1, 2):
                    c_a(w, s, d, kind).wait_send()
    for w in range(AHEAD, waves):
        for c in xb_outs(w):
            c.wait()
        for s in (0, 1):
            for d in (0, 1):
                c_e(w, s, d).wait_recv()
                c_e(w, s, d).wait_send()
    done = [pltpu.make_async_copy(whole.at[w], dx_h.at[pl.ds(w * wave, wave)], o_sem.at[w % 2]) for w in range(AHEAD)]
    for w in (waves - 2, waves - 1):
        for c in outs(w):
            c.wait()
        tile_out(tiles - waves + w).wait()
        for s in (0, 1):
            for d in (0, 1):
                c_h1(w, s, d).wait_send()
                c_n(w, s, d).wait_send()
                c_g1(w, s, d).wait_send()
                c_gn(w, s, d).wait_send()
    for c in done:
        c.start()
    for c in done:
        c.wait()


def reduce_terms(side, dy, gate, up, w_gate, w_up, w_down):
    rows, depth = dy.shape
    ff = gate.shape[1]
    wave, half = WAVE, WAVE // 2
    block = depth // (2 * side)
    sub = block // side
    any_ = pl.BlockSpec(memory_space=pl.ANY)
    waves = rows // wave
    piece = jax.ShapeDtypeStruct((2, waves - AHEAD, half, block), BF)
    V, DMA = pltpu.VMEM, pltpu.SemaphoreType.DMA
    return pl.pallas_call(
        functools.partial(reduce_kernel, side),
        out_shape=[jax.ShapeDtypeStruct((rows, 2 * ff), BF), jax.ShapeDtypeStruct((ff, depth), BF),
                   jax.ShapeDtypeStruct((AHEAD * wave, depth), BF), piece, piece, piece, piece],
        in_specs=[any_] * 6,
        out_specs=[any_] * 7,
        scratch_shapes=[
            V((ff, depth), BF), V((depth, 2 * ff), BF), V((2, wave, depth), BF), V((2, wave, ff), BF), V((2, wave, ff), BF),
            V((4, wave, 2 * ff), BF), V((rows, ff), BF),
            V((2, 2, wave, block), BF), V((2, 2, 2, wave, block), BF), V((4, 2, 2, half, block), BF), V((4, 2, 2, wave, block), BF),
            V((4, 2, wave, block), F32),
            V((2, 2, wave, sub), BF), V((2, 2, 2, wave, sub), BF), V((4, 2, 2, half, sub), BF), V((4, 2, 2, wave, sub), BF),
            V((waves, 2, wave, block), BF), V((AHEAD, wave, depth), BF),
            DMA((3, side, 2)), DMA((2, 3)), DMA((2,)), DMA((waves, 2, 2)),
            DMA((2, 2, 2)), DMA((2, 2, 2)), DMA((2, 2, 2)), DMA((2, 2, 2)), DMA((waves, 2, 2)), DMA((waves, 2, 2)),
            DMA((4, 2, 2)), DMA((4, 2, 2)), DMA((4, 2, 2)), DMA((4, 2, 2)), DMA((waves, 2, 2)), DMA((waves, 2, 2)),
            DMA((AHEAD, 2, 2, 3)), DMA((AHEAD, 2, 2, 3)), DMA((waves, 2, 2)), DMA((waves, 2, 2)), DMA((2, rows // ff)), DMA((2,)),
        ],
        compiler_params=pltpu.CompilerParams(collective_id=0, has_side_effects=True, vmem_limit_bytes=VMEM_LIMIT),
        cost_estimate=pl.CostEstimate(flops=6 * rows * depth * ff, bytes_accessed=2 * (rows * depth + 7 * rows * ff + 3 * ff * depth), transcendentals=0),
        name="reduce_terms",
    )(dy, gate, up, w_gate, w_up, w_down)


def copies(side, parts, where, dx, buf, sem):
    me = lax.axis_index("tp")
    pos = (lax.div(me, side), lax.rem(me, side))
    block = buf.shape[-1]
    got, put = [], []
    for k, (src, (s, part, d)) in enumerate(zip(parts, where)):
        col = (s * side + lax.rem(pos[s] + d + side, side)) * block
        dst = dx.at[pl.ds(AHEAD, buf.shape[1]), part, :, pl.ds(pl.multiple_of(col, block), block)]
        got.append(pltpu.make_async_copy(src, buf.at[k], sem.at[0, k]))
        put.append(pltpu.make_async_copy(buf.at[k], dst, sem.at[1, k]))
    return got, put


def split(arrays):
    return [a.at[k] for a in arrays for k in (0, 1)]


HERE = [k for s in (0, 1) for d, step in enumerate((1, -1)) for k in ((s, 1 - d, 0), (s, d, -step))]
THERE = [k for s in (0, 1) for d, step in enumerate((1, -1)) for k in ((s, 1 - d, -step), (s, d, 2))]


def products_kernel(side, x, dgu, dwd_in, dx_in, a0, a1, b0, b1, og, ou, dwd, dx, w_buf, r_buf, buf, w_sem, sem):
    ff = og.shape[1]
    i = pl.program_id(0)
    got, put = copies(side, split((a0, a1, b0, b1)), HERE, dx, buf, sem)
    h = ff // 2
    for k in (0, 1):
        r = pl.ds(k * h, h)
        got.append(pltpu.make_async_copy(dwd_in.at[r], w_buf.at[r], w_sem.at[0, k]))
        put.append(pltpu.make_async_copy(w_buf.at[r], dwd.at[r], w_sem.at[1, k]))
    got.append(pltpu.make_async_copy(dx_in, r_buf, w_sem.at[0, 2]))
    put.append(pltpu.make_async_copy(r_buf, dx.at[pl.ds(0, AHEAD)], w_sem.at[1, 2]))

    @pl.when(i == 1)
    def _():
        for c in got:
            c.start()

    @pl.when(i == 3)
    def _():
        for c, p in zip(got, put):
            c.wait()
            p.start()
    xt = x[...].T
    og[...] = jnp.dot(xt, dgu[:, 0:ff], preferred_element_type=F32).astype(BF)
    ou[...] = jnp.dot(xt, dgu[:, ff:2 * ff], preferred_element_type=F32).astype(BF)

    @pl.when(i == pl.num_programs(0) - 1)
    def _():
        for p in put:
            p.wait()


ANY = pl.BlockSpec(memory_space=pl.ANY)


def products(side, x, dgu, dwd, dx_rows, arrays):
    rows, depth = x.shape
    ff = dgu.shape[1] // 2
    dx_rows = dx_rows.reshape(AHEAD, 2, WAVE // 2, depth)
    return pl.pallas_call(
        functools.partial(products_kernel, side),
        grid=(depth // TILE,),
        in_specs=[pl.BlockSpec((rows, TILE), lambda i: (0, i)), pl.BlockSpec((rows, 2 * ff), lambda i: (0, 0))] + [ANY] * 6,
        out_specs=[pl.BlockSpec((TILE, ff), lambda i: (i, 0))] * 2 + [ANY] * 2,
        out_shape=[jax.ShapeDtypeStruct((depth, ff), BF)] * 2
        + [jax.ShapeDtypeStruct(dwd.shape, BF), jax.ShapeDtypeStruct((rows // WAVE, 2, WAVE // 2, depth), BF)],
        scratch_shapes=[pltpu.VMEM(dwd.shape, BF), pltpu.VMEM(dx_rows.shape, BF), pltpu.VMEM((8, *arrays[0].shape[1:]), BF),
                        pltpu.SemaphoreType.DMA((2, 3)), pltpu.SemaphoreType.DMA((2, 8))],
        cost_estimate=pl.CostEstimate(flops=4 * rows * depth * ff, bytes_accessed=4 * (2 * rows * depth + 2 * rows * ff + 2 * depth * ff), transcendentals=0),
        compiler_params=pltpu.CompilerParams(vmem_limit_bytes=VMEM_LIMIT),
        name="products",
    )(x, dgu, dwd, dx_rows, *arrays)


def finish_kernel(side, a0, a1, b0, b1, _, dx, buf, sem):
    got, put = copies(side, split((a0, a1, b0, b1)), THERE, dx, buf, sem)
    for c in got:
        c.start()
    for c, p in zip(got, put):
        c.wait()
        p.start()
    for p in put:
        p.wait()


def finish(side, dx, arrays):
    return pl.pallas_call(
        functools.partial(finish_kernel, side),
        in_specs=[ANY] * 5,
        out_specs=ANY,
        out_shape=jax.ShapeDtypeStruct(dx.shape, BF),
        input_output_aliases={4: 0},
        scratch_shapes=[pltpu.VMEM((8, *arrays[0].shape[1:]), BF), pltpu.SemaphoreType.DMA((2, 8))],
        cost_estimate=pl.CostEstimate(flops=1000000, bytes_accessed=16 * arrays[0].size, transcendentals=0),
        compiler_params=pltpu.CompilerParams(vmem_limit_bytes=VMEM_LIMIT),
        name="finish",
    )(*arrays, dx)


def solution(mesh):
    size = mesh.shape["tp"]
    side = math.isqrt(size)

    def ring(axis, d):
        def to(i):
            x, y = divmod(i, side)
            return ((x + d) % side) * side + y if axis == 0 else x * side + (y + d) % side
        return [(i, to(i)) for i in range(size)]

    def step(x, dy, gate, up, w_gate, w_up, w_down):
        dgu, dw_down, dx_rows, *here = reduce_terms(side, dy, gate, up, w_gate, w_up, w_down)
        there = [lax.ppermute(v, "tp", perm=ring(k // 2, 1 - k % 2 * 2)) for k, v in enumerate(here)]
        dw_gate, dw_up, dw_down, dx = products(side, x, dgu, dw_down, dx_rows, here)
        dx = finish(side, dx, there).reshape(x.shape)
        return dx, dw_gate, dw_up, dw_down

    tokens, columns, rows = P("dp", None), P(None, "tp"), P("tp", None)
    return jax.shard_map(
        step,
        mesh=mesh,
        in_specs=(tokens, tokens, P("dp", "tp"), P("dp", "tp"), columns, columns, rows),
        out_specs=(tokens, P("dp", "tp"), P("dp", "tp"), P(("dp", "tp"), None)),
        check_vma=False,
    )
```

```python
import functools
import math

import jax
import jax.numpy as jnp
from jax import lax
from jax.experimental import pallas as pl
from jax.experimental.pallas import tpu as pltpu
from jax.sharding import PartitionSpec as P

MESH = pl.DeviceIdType.MESH
BF, F32 = jnp.bfloat16, jnp.float32
NT = (((1,), (1,)), ((), ()))
VMEM_LIMIT = 63 * 1024 * 1024
WAVE = 256
TILE = 512
PRODUCTS_LIMIT = VMEM_LIMIT


def reduce_kernel(side, dy_h, gate_h, up_h, wg_h, wu_h, wd_h, dgu_h, dwd_h, a0_h, a1_h, b0_h, b1_h,
                  wd, wgu, dy, gate, up, dgu, hid, s_h1, s_n, r_h1, r_n, total, s_g1, s_gn, r_g1, r_gn, xb,
                  w_sem, in_sem, o_sem, xo_sem, ss_h1, ss_n, ss_g1, ss_gn, ss_f, ss_w, rs_h1, rs_n, rs_g1, rs_gn, rs_f, rs_w,
                  ss_e, rs_e, t_sem, u_sem):
    rows, depth = dy_h.shape
    ff = gate_h.shape[1]
    wave = dy.shape[1]
    half = wave // 2
    waves = rows // wave
    pass_on = ((a0_h, a1_h), (b0_h, b1_h))
    block = depth // (2 * side)
    sub = block // side
    me = lax.axis_index("tp")
    px, py = lax.div(me, side), lax.rem(me, side)
    first, second = (px, py), (py, px)

    def at(pos, d):
        return lax.rem(pos + d + side, side)

    def peer(axis, d):
        return {"tp": at(px, d) * side + py if axis == 0 else px * side + at(py, d)}

    TOP, BOT = pl.ds(0, half), pl.ds(half, half)
    HALVES = (TOP, BOT)
    STEP = (1, -1)

    def remote(src, dst, ss, rs, axis, d):
        return pltpu.make_async_remote_copy(src_ref=src, dst_ref=dst, send_sem=ss, recv_sem=rs,
                                            device_id=peer(axis, STEP[d]), device_id_type=MESH)

    def c_h1(w, s, d):
        return remote(s_h1.at[w % 2, s, HALVES[d]], r_h1.at[w % 4, s, d], ss_h1.at[w % 2, s, d], rs_h1.at[w % 4, s, d], s, d)

    def c_n(w, s, d):
        return remote(s_n.at[w % 2, s, d], r_n.at[w % 4, s, d], ss_n.at[w % 2, s, d], rs_n.at[w % 4, s, d], s, d)

    def c_g1(w, s, d):
        return remote(s_g1.at[w % 2, s, HALVES[d]], r_g1.at[w % 4, s, d], ss_g1.at[w % 2, s, d], rs_g1.at[w % 4, s, d], 1 - s, d)

    def c_gn(w, s, d):
        return remote(s_gn.at[w % 2, s, d], r_gn.at[w % 4, s, d], ss_gn.at[w % 2, s, d], rs_gn.at[w % 4, s, d], 1 - s, d)

    def cols(s, d):
        return pl.ds(pl.multiple_of(at(second[s], d) * sub, sub), sub)

    def c_f(w, s, d):
        own = xb.at[w, s, :, cols(s, 0)]
        return remote(own, own, ss_f.at[w, s, d], rs_f.at[w, s, d], 1 - s, d)

    def c_w(w, s, d):
        got = xb.at[w, s, HALVES[d], cols(s, -STEP[d])]
        return remote(got, got, ss_w.at[w, s, d], rs_w.at[w, s, d], 1 - s, d)

    def ins(w):
        r = pl.ds(pl.multiple_of(w * wave, wave), wave)
        k = w % 2
        return (pltpu.make_async_copy(dy_h.at[r], dy.at[k], in_sem.at[k, 0]),
                pltpu.make_async_copy(gate_h.at[r], gate.at[k], in_sem.at[k, 1]),
                pltpu.make_async_copy(up_h.at[r], up.at[k], in_sem.at[k, 2]))

    def outs(w):
        r = pl.ds(pl.multiple_of(w * wave, wave), wave)
        return (pltpu.make_async_copy(dgu.at[w % 4], dgu_h.at[r], o_sem.at[w % 2]),)

    def xb_outs(w):
        return [pltpu.make_async_copy(xb.at[w, s, HALVES[1 - d]], pass_on[s][d].at[0, w], xo_sem.at[w, s, d])
                for s in (0, 1) for d in (0, 1)]

    def c_e(w, s, d):
        return remote(xb.at[w, s, HALVES[d]], pass_on[s][d].at[1, w], ss_e.at[w, s, d], rs_e.at[w, s, d], s, d)

    def weights(s, d):
        r = pl.ds(pl.multiple_of(s * side * block + at(first[s], d) * block, block), block)
        k = (d + side) % side
        return (pltpu.make_async_copy(wg_h.at[r], wgu.at[r, pl.ds(0, ff)], w_sem.at[s, k, 0]),
                pltpu.make_async_copy(wu_h.at[r], wgu.at[r, pl.ds(ff, ff)], w_sem.at[s, k, 1]))

    parts = 2
    part = ff // parts

    def down(c):
        r = pl.ds(c * part, part)
        return pltpu.make_async_copy(wd_h.at[r], wd.at[r], w_sem.at[2, 0, c])

    for c in ins(0):
        c.start()
    for p in range(parts):
        down(p).start()
    for s in (0, 1):
        for c in weights(s, 2):
            c.start()

    barrier = pltpu.get_barrier_semaphore()
    for axis in (0, 1):
        for d in (1, -1):
            pl.semaphore_signal(barrier, inc=1, device_id=peer(axis, d), device_id_type=MESH)
    pl.semaphore_wait(barrier, 4)

    tiles = depth // TILE

    def tile_in(j):
        c = pl.ds(pl.multiple_of(j * TILE, TILE), TILE)
        return [pltpu.make_async_copy(dy_h.at[pl.ds(i * ff, ff), c], wd.at[:, tile_at(j, i)], t_sem.at[j % 2, i]) for i in range(rows // ff)]

    def tile_at(j, i):
        return pl.ds(pl.multiple_of(((j % 2) * (rows // ff) + i) * TILE, TILE), TILE)

    def tile_out(j):
        c = pl.ds(pl.multiple_of(j * TILE, TILE), TILE)
        return pltpu.make_async_copy(wd.at[:, out_at(j)], dwd_h.at[:, c], u_sem.at[j % 2])

    def out_at(j):
        return pl.ds(pl.multiple_of((2 * (rows // ff) + j % 2) * TILE, TILE), TILE)

    def dot_block(w, s, d):
        r = pl.ds(pl.multiple_of(s * side * block + at(first[s], d) * block, block), block)
        return lax.dot_general(dgu[w % 4], wgu[r, :], NT, preferred_element_type=F32)

    def wait_weights(t, when, d):
        @pl.when(t == when)
        def _():
            for s in (0, 1):
                for c in weights(s, d):
                    c.wait()

    def stage(t, lag):
        w = t - lag
        return w, pl.when(jnp.logical_and(w >= 0, w < waves))

    def body(t, _):
        w0, active = stage(t, 0)

        @active
        def _():
            @pl.when(w0 + 1 < waves)
            def _():
                for c in ins(w0 + 1):
                    c.start()
            for c in ins(w0):
                c.wait()

            @pl.when(w0 >= 2)
            def _():
                for c in outs(w0 - 2):
                    c.wait()
            k = w0 % 2
            for p in range(parts):
                @pl.when(w0 == 0)
                def _():
                    down(p).wait()
                    if p == 0:
                        for d in (1, -1, 0):
                            for s in (0, 1):
                                for c in weights(s, d):
                                    c.start()
                f = pl.ds(p * part, part)
                dh = lax.dot_general(dy[k], wd[f, :], NT, preferred_element_type=F32)
                g, u = gate[k, :, f].astype(F32), up[k, :, f].astype(F32)
                sg = jax.nn.sigmoid(g)
                si = g * sg
                dgu[w0 % 4, :, f] = (dh * u * (sg * (1.0 + g * (1.0 - sg)))).astype(BF)
                dgu[w0 % 4, :, pl.ds(ff + p * part, part)] = (dh * si).astype(BF)
                hid[pl.ds(pl.multiple_of(w0 * wave, wave), wave), f] = (si * u).astype(BF)
            for c in outs(w0):
                c.start()

            @pl.when(w0 == waves - 1)
            def _():
                for c in tile_in(0):
                    c.start()

        @stage(t, 0)[1]
        def _():
            wait_weights(t, 0, 2)
            for s in (0, 1):
                @pl.when(w0 >= 2)
                def _():
                    for d in (0, 1):
                        c_h1(w0 - 2, s, d).wait_send()
                s_h1[w0 % 2, s] = dot_block(w0, s, 2).astype(BF)
                for d in (0, 1):
                    c_h1(w0, s, d).start()

        w1, active = stage(t, 1)

        @active
        def _():
            wait_weights(t, 1, 1)
            wait_weights(t, 1, -1)
            for d in (0, 1):
                for s in (0, 1):
                    @pl.when(w1 >= 2)
                    def _():
                        c_n(w1 - 2, s, d).wait_send()
                    term = dot_block(w1, s, STEP[d])
                    c_h1(w1, s, d).wait_recv()
                    got, other = HALVES[d], HALVES[1 - d]
                    s_n[w1 % 2, s, d, got] = (term[d * half:(d + 1) * half] + r_h1[w1 % 4, s, d].astype(F32)).astype(BF)
                    s_n[w1 % 2, s, d, other] = term[(1 - d) * half:(2 - d) * half].astype(BF)
                    c_n(w1, s, d).start()

        w2, active = stage(t, 2)

        @active
        def _():
            wait_weights(t, 2, 0)
            for s in (0, 1):
                @pl.when(w2 >= 2)
                def _():
                    for d in (0, 1):
                        c_g1(w2 - 2, s, d).wait_send()
                term = dot_block(w2, s, 0)
                for d in (0, 1):
                    c_n(w2, s, d).wait_recv()
                total[w2 % 4, s] = term + (r_n[w2 % 4, s, 0].astype(F32) + r_n[w2 % 4, s, 1].astype(F32))
                s_g1[w2 % 2, s] = total[w2 % 4, s, :, cols(s, 2)].astype(BF)
                for d in (0, 1):
                    c_g1(w2, s, d).start()

        w3, active = stage(t, 3)

        @active
        def _():
            for s in (0, 1):
                for d in (0, 1):
                    @pl.when(w3 >= 2)
                    def _():
                        c_gn(w3 - 2, s, d).wait_send()
                    c_g1(w3, s, d).wait_recv()
                    got, other = HALVES[d], HALVES[1 - d]
                    where = cols(s, STEP[d])
                    s_gn[w3 % 2, s, d, got] = (total[w3 % 4, s, got, where] + r_g1[w3 % 4, s, d].astype(F32)).astype(BF)
                    s_gn[w3 % 2, s, d, other] = total[w3 % 4, s, other, where].astype(BF)
                    c_gn(w3, s, d).start()

        w4, active = stage(t, 4)

        @active
        def _():
            for s in (0, 1):
                for d in (0, 1):
                    c_gn(w4, s, d).wait_recv()
                xb[w4, s, :, cols(s, 0)] = (
                    total[w4 % 4, s, :, cols(s, 0)] + (r_gn[w4 % 4, s, 0].astype(F32) + r_gn[w4 % 4, s, 1].astype(F32))).astype(BF)
                for d in (0, 1):
                    c_f(w4, s, d).start()

        w5, active = stage(t, 5)

        @active
        def _():
            for s in (0, 1):
                for d in (0, 1):
                    c_f(w5, s, d).wait_recv()
                for d in (0, 1):
                    c_w(w5, s, d).start()

        w6, active = stage(t, 6)

        @active
        def _():
            for s in (0, 1):
                for d in (0, 1):
                    c_w(w6, s, d).wait_recv()
                    c_w(w6, s, d).wait_send()
                    c_f(w6, s, d).wait_send()

            for c in xb_outs(w6):
                c.start()

        w7, active = stage(t, 7)

        @active
        def _():
            for s in (0, 1):
                for d in (0, 1):
                    c_e(w7, s, d).start()

        j = t - waves

        @pl.when(jnp.logical_and(j >= 0, j < tiles))
        def _():
            for c in tile_in(j):
                c.wait()

            @pl.when(j + 1 < tiles)
            def _():
                for c in tile_in(j + 1):
                    c.start()

            @pl.when(j >= 2)
            def _():
                tile_out(j - 2).wait()
            acc = 0
            for i in range(rows // ff):
                acc += lax.dot_general(hid[pl.ds(i * ff, ff), :], wd[:, tile_at(j, i)], (((0,), (0,)), ((), ())), preferred_element_type=F32)
            wd[:, out_at(j)] = acc.astype(BF)
            tile_out(j).start()
        return 0

    lax.fori_loop(0, waves + max(8, tiles), body, 0)
    for w in range(waves):
        for c in xb_outs(w):
            c.wait()
        for s in (0, 1):
            for d in (0, 1):
                c_e(w, s, d).wait_recv()
                c_e(w, s, d).wait_send()
    for w in (waves - 2, waves - 1):
        for c in outs(w):
            c.wait()
        tile_out(tiles - waves + w).wait()
        for s in (0, 1):
            for d in (0, 1):
                c_h1(w, s, d).wait_send()
                c_n(w, s, d).wait_send()
                c_g1(w, s, d).wait_send()
                c_gn(w, s, d).wait_send()


def reduce_terms(side, dy, gate, up, w_gate, w_up, w_down):
    rows, depth = dy.shape
    ff = gate.shape[1]
    wave, half = WAVE, WAVE // 2
    block = depth // (2 * side)
    sub = block // side
    any_ = pl.BlockSpec(memory_space=pl.ANY)
    waves = rows // wave
    piece = jax.ShapeDtypeStruct((2, waves, half, block), BF)
    V, DMA = pltpu.VMEM, pltpu.SemaphoreType.DMA
    return pl.pallas_call(
        functools.partial(reduce_kernel, side),
        out_shape=[jax.ShapeDtypeStruct((rows, 2 * ff), BF), jax.ShapeDtypeStruct((ff, depth), BF),
                   piece, piece, piece, piece],
        in_specs=[any_] * 6,
        out_specs=[any_] * 6,
        scratch_shapes=[
            V((ff, depth), BF), V((depth, 2 * ff), BF), V((2, wave, depth), BF), V((2, wave, ff), BF), V((2, wave, ff), BF),
            V((4, wave, 2 * ff), BF), V((rows, ff), BF),
            V((2, 2, wave, block), BF), V((2, 2, 2, wave, block), BF), V((4, 2, 2, half, block), BF), V((4, 2, 2, wave, block), BF),
            V((4, 2, wave, block), F32),
            V((2, 2, wave, sub), BF), V((2, 2, 2, wave, sub), BF), V((4, 2, 2, half, sub), BF), V((4, 2, 2, wave, sub), BF),
            V((waves, 2, wave, block), BF),
            DMA((3, side, 4)), DMA((2, 3)), DMA((2,)), DMA((waves, 2, 2)),
            DMA((2, 2, 2)), DMA((2, 2, 2)), DMA((2, 2, 2)), DMA((2, 2, 2)), DMA((waves, 2, 2)), DMA((waves, 2, 2)),
            DMA((4, 2, 2)), DMA((4, 2, 2)), DMA((4, 2, 2)), DMA((4, 2, 2)), DMA((waves, 2, 2)), DMA((waves, 2, 2)),
            DMA((waves, 2, 2)), DMA((waves, 2, 2)), DMA((2, rows // ff)), DMA((2,)),
        ],
        compiler_params=pltpu.CompilerParams(collective_id=0, has_side_effects=True, vmem_limit_bytes=VMEM_LIMIT),
        cost_estimate=pl.CostEstimate(flops=6 * rows * depth * ff, bytes_accessed=2 * (rows * depth + 7 * rows * ff + 3 * ff * depth), transcendentals=0),
        name="reduce_terms",
    )(dy, gate, up, w_gate, w_up, w_down)


def copies(side, parts, where, dx, sem, buf=None):
    me = lax.axis_index("tp")
    pos = (lax.div(me, side), lax.rem(me, side))
    block = dx.shape[-1] // (2 * side)
    got, put = [], []
    for k, (src, (s, part, d)) in enumerate(zip(parts, where)):
        col = (s * side + lax.rem(pos[s] + d + side, side)) * block
        dst = dx.at[:, part, :, pl.ds(pl.multiple_of(col, block), block)]
        if buf is not None:
            got.append(pltpu.make_async_copy(src, buf.at[k], sem.at[0, k]))
            src = buf.at[k]
        put.append(pltpu.make_async_copy(src, dst, sem.at[1, k]))
    return got, put


def split(arrays):
    return [a.at[k] for a in arrays for k in (0, 1)]


HERE = [k for s in (0, 1) for d, step in enumerate((1, -1)) for k in ((s, 1 - d, 0), (s, d, -step))]
THERE = [k for s in (0, 1) for d, step in enumerate((1, -1)) for k in ((s, 1 - d, -step), (s, d, 2))]


def products_kernel(side, x, dgu_h, dwd_in, a0, a1, b0, b1, og, ou, dwd, dx, dgu, w_buf, buf, w_sem, sem, g_sem):
    ff = og.shape[1]
    i = pl.program_id(0)
    got, put = copies(side, split((a0, a1, b0, b1)), HERE, dx, sem, buf)
    h = ff // 2
    for k in (0, 1):
        r = pl.ds(k * h, h)
        got.append(pltpu.make_async_copy(dwd_in.at[r], w_buf.at[r], w_sem.at[0, k]))
        put.append(pltpu.make_async_copy(w_buf.at[r], dwd.at[r], w_sem.at[1, k]))

    @pl.when(i == 0)
    def _():
        n = x.shape[0] // PARTS
        rows = [pl.ds(k * n, n) for k in range(PARTS)]
        ins = [pltpu.make_async_copy(dgu_h.at[r], dgu.at[r], g_sem.at[k]) for k, r in enumerate(rows)]
        for c in ins:
            c.start()
        g = u = 0.0
        for r, c in zip(rows, ins):
            xt = x[r, :].T
            c.wait()
            g += jnp.dot(xt, dgu[r, 0:ff], preferred_element_type=F32)
            u += jnp.dot(xt, dgu[r, ff:2 * ff], preferred_element_type=F32)
        og[...] = g.astype(BF)
        ou[...] = u.astype(BF)

    @pl.when(i == 1)
    def _():
        for c in got:
            c.start()

    @pl.when(i == 3)
    def _():
        for c, p in zip(got, put):
            c.wait()
            p.start()

    @pl.when(i > 0)
    def _():
        xt = x[...].T
        og[...] = jnp.dot(xt, dgu[:, 0:ff], preferred_element_type=F32).astype(BF)
        ou[...] = jnp.dot(xt, dgu[:, ff:2 * ff], preferred_element_type=F32).astype(BF)

    @pl.when(i == pl.num_programs(0) - 1)
    def _():
        for p in put:
            p.wait()


ANY = pl.BlockSpec(memory_space=pl.ANY)
PARTS = 4


def products(side, x, dgu, dwd, arrays):
    rows, depth = x.shape
    ff = dgu.shape[1] // 2
    return pl.pallas_call(
        functools.partial(products_kernel, side),
        grid=(depth // TILE,),
        in_specs=[pl.BlockSpec((rows, TILE), lambda i: (0, i))] + [ANY] * 6,
        out_specs=[pl.BlockSpec((TILE, ff), lambda i: (i, 0))] * 2 + [ANY] * 2,
        out_shape=[jax.ShapeDtypeStruct((depth, ff), BF)] * 2
        + [jax.ShapeDtypeStruct(dwd.shape, BF), jax.ShapeDtypeStruct((rows // WAVE, 2, WAVE // 2, depth), BF)],
        scratch_shapes=[pltpu.VMEM(dgu.shape, BF), pltpu.VMEM(dwd.shape, BF), pltpu.VMEM((8, *arrays[0].shape[1:]), BF),
                        pltpu.SemaphoreType.DMA((2, 2)), pltpu.SemaphoreType.DMA((2, 8)), pltpu.SemaphoreType.DMA((PARTS,))],
        cost_estimate=pl.CostEstimate(flops=4 * rows * depth * ff, bytes_accessed=4 * (2 * rows * depth + 2 * rows * ff + 2 * depth * ff), transcendentals=0),
        compiler_params=pltpu.CompilerParams(vmem_limit_bytes=PRODUCTS_LIMIT),
        name="products",
    )(x, dgu, dwd, *arrays)


def finish_kernel(side, a0, a1, b0, b1, _, dx, buf, sem):
    got, put = copies(side, split((a0, a1, b0, b1)), THERE, dx, sem, buf)
    for c in got:
        c.start()
    for c, p in zip(got, put):
        c.wait()
        p.start()
    for p in put:
        p.wait()


def finish(side, dx, arrays):
    return pl.pallas_call(
        functools.partial(finish_kernel, side),
        in_specs=[ANY] * 5,
        out_specs=ANY,
        out_shape=jax.ShapeDtypeStruct(dx.shape, BF),
        input_output_aliases={4: 0},
        scratch_shapes=[pltpu.VMEM((8, *arrays[0].shape[1:]), BF), pltpu.SemaphoreType.DMA((2, 8))],
        cost_estimate=pl.CostEstimate(flops=1000000, bytes_accessed=16 * arrays[0].size, transcendentals=0),
        compiler_params=pltpu.CompilerParams(vmem_limit_bytes=PRODUCTS_LIMIT),
        name="finish",
    )(*arrays, dx)


def solution(mesh):
    size = mesh.shape["tp"]
    side = math.isqrt(size)

    def ring(axis, d):
        def to(i):
            x, y = divmod(i, side)
            return ((x + d) % side) * side + y if axis == 0 else x * side + (y + d) % side
        return [(i, to(i)) for i in range(size)]

    def step(x, dy, gate, up, w_gate, w_up, w_down):
        dgu, dw_down, *here = reduce_terms(side, dy, gate, up, w_gate, w_up, w_down)
        there = [lax.ppermute(v, "tp", perm=ring(k // 2, 1 - k % 2 * 2)) for k, v in enumerate(here)]
        dw_gate, dw_up, dw_down, dx = products(side, x, dgu, dw_down, here)
        dx = finish(side, dx, there).reshape(x.shape)
        return dx, dw_gate, dw_up, dw_down

    tokens, columns, rows = P("dp", None), P(None, "tp"), P("tp", None)
    return jax.shard_map(
        step,
        mesh=mesh,
        in_specs=(tokens, tokens, P("dp", "tp"), P("dp", "tp"), columns, columns, rows),
        out_specs=(tokens, P("dp", "tp"), P("dp", "tp"), P(("dp", "tp"), None)),
        check_vma=False,
    )
```
